256 devices in a mesh: wide: 32 (over z, x), group: 8 (over y, core).
Axes of the slice: x: 4, y: 4, z: 8, core: 2. Of those that a mesh axis runs over, the one named last changes fastest.
Arguments:
- feat4: bfloat16 [256, 24, 24, 256], P(('wide', 'group')), may hold values from -100 to 100
- feat5: bfloat16 [256, 12, 12, 256], P(('wide', 'group')), may hold values from -100 to 100
- feat6: bfloat16 [256, 6, 6, 256], P(('wide', 'group')), may hold values from -100 to 100
- feat7: bfloat16 [256, 3, 3, 256], P(('wide', 'group')), may hold values from -100 to 100
- out_grad4: bfloat16 [256, 24, 24, 256], P(('wide', 'group')), may hold values from -6 to 6
- out_grad5: bfloat16 [256, 12, 12, 256], P(('wide', 'group')), may hold values from -6 to 6
- out_grad6: bfloat16 [256, 6, 6, 256], P(('wide', 'group')), may hold values from -6 to 6
- out_grad7: bfloat16 [256, 3, 3, 256], P(('wide', 'group')), may hold values from -6 to 6
- conv_weight: bfloat16 [3, 3, 256, 256], replicated, may hold values from -0.125 to 0.125
- bn_gain: float32 [4, 256], replicated, may hold values from 0.25 to 1.75
- bn_shift: float32 [4, 256], replicated, may hold values from -0.5 to 0.5
- heights: int32 [256], P(('wide', 'group')), may hold values from 168 to 384
- widths: int32 [256], P(('wide', 'group')), may hold values from 168 to 384
Outputs:
- out4: bfloat16 [256, 24, 24, 256], P(('wide', 'group'))
- out5: bfloat16 [256, 12, 12, 256], P(('wide', 'group'))
- out6: bfloat16 [256, 6, 6, 256], P(('wide', 'group'))
- out7: bfloat16 [256, 3, 3, 256], P(('wide', 'group'))
- d_feat4: bfloat16 [256, 24, 24, 256], P(('wide', 'group'))
- d_feat5: bfloat16 [256, 12, 12, 256], P(('wide', 'group'))
- d_feat6: bfloat16 [256, 6, 6, 256], P(('wide', 'group'))
- d_feat7: bfloat16 [256, 3, 3, 256], P(('wide', 'group'))
- d_weight: float32 [3, 3, 256, 256], replicated
- d_gain: float32 [4, 256], replicated
- d_shift: float32 [4, 256], replicated
The draws below stay inside these ranges and needn't reach their ends.
Inputs may be any that keep to these rules, and one draw needn't show every extreme that they name: `heights`: pixel height of the valid part of each image. `widths`: pixel width of the valid part of each image.
All inputs are finite; a program needn't handle non-finite values.
Results may differ from the reference program's by a relative error of at most 0.0049.
Values sent between devices are 32-bit elements; how exact they have to be, the bound alone decides.
A program may use at most 64 MiB of HBM per device.

```python
from functools import partial
import jax
import jax.numpy as jnp
from jax import lax

CH = 256
SIDE4 = 24
LEVELS = 4
SIDE5 = 12
SIDE6 = 6
SIDE7 = 3
IMAGES = 256


def feature_values(key, extent):
    noise_key, offset_key = jax.random.split(key, 2)
    places = jnp.arange(IMAGES, dtype=jnp.float32) / max(IMAGES - 1, 1)
    image_ramp = 1.0 + 2.0 * places
    noise_part = jnp.clip(jax.random.normal(noise_key, (IMAGES, extent, extent, CH), jnp.float32), -6.0, 6.0)
    offset = jax.random.uniform(offset_key, (IMAGES, 1, 1, CH), jnp.float32, -0.5, 1.0)
    values = image_ramp[:, None, None, None] * (noise_part + offset)
    return values.astype(jnp.bfloat16)


def draw_feat4(key, part):
    return feature_values(jax.random.fold_in(key, 4), SIDE4)


def draw_feat5(key, part):
    return feature_values(jax.random.fold_in(key, 5), SIDE5)


def draw_feat6(key, part):
    return feature_values(jax.random.fold_in(key, 6), SIDE6)


def draw_feat7(key, part):
    return feature_values(jax.random.fold_in(key, 7), SIDE7)


def place_ends(entries, own_key, smallest, top_value):
    longest = entries.shape.index(max(entries.shape))
    spots = []
    for shift in (0, 1):
        where = [jax.random.randint(jax.random.fold_in(own_key, axis), (), 0, length) for axis, length in enumerate(entries.shape)]
        where[longest] = (where[longest] + shift) % entries.shape[longest]
        spots.append(tuple(where))
    return entries.at[spots[0]].set(smallest).at[spots[1]].set(top_value)


def block_levels(stream_key, shape, shards, smallest, largest):
    level = 1.0
    for position, parts in shards:
        draws = jax.random.uniform(jax.random.fold_in(jax.random.fold_in(stream_key, 6), position), (parts,), jnp.float32, smallest / len(shards), largest / len(shards))
        level = level * jnp.repeat(jnp.exp(draws), shape[position] // parts).reshape((-1,) + (1,) * (len(shape) - 1 - position))
    return level


def bell_draw(key, dims, spread, bound, cuts=(), held_as=jnp.bfloat16):
    entries = jax.random.normal(key, dims, jnp.float32) * spread
    if len(cuts) > 0:
        entries = block_levels(key, dims, cuts, -0.22, 0.18) * entries
    return jnp.clip(entries, min=-bound, max=bound).astype(held_as)


def setup_inputs(seed: int = 0) -> dict:
    streams_of = jax.random.split(jax.random.key(seed), 14)
    feat4 = draw_feat4(jax.random.fold_in(streams_of[13], 71), 0)
    feat5 = draw_feat5(jax.random.fold_in(streams_of[13], 71), 0)
    feat6 = draw_feat6(jax.random.fold_in(streams_of[13], 71), 0)
    feat7 = draw_feat7(jax.random.fold_in(streams_of[13], 71), 0)
    out_grad4 = bell_draw(streams_of[4], (IMAGES, SIDE4, SIDE4, CH), 1.0, 6.0, ((0, 256),))
    out_grad5 = bell_draw(streams_of[5], (IMAGES, SIDE5, SIDE5, CH), 1.0, 6.0, ((0, 256),))
    out_grad6 = bell_draw(streams_of[6], (IMAGES, SIDE6, SIDE6, CH), 1.0, 6.0, ((0, 256),))
    out_grad7 = bell_draw(streams_of[7], (IMAGES, SIDE7, SIDE7, CH), 1.0, 6.0, ((0, 256),))
    conv_weight = bell_draw(streams_of[8], (3, 3, CH, CH), (9 * CH) ** -0.5, 0.125)
    bn_gain = jnp.clip(1.0 + 0.15 * jax.random.normal(streams_of[9], (LEVELS, CH), jnp.float32), 0.25, 1.75)
    bn_shift = jnp.clip(jax.random.uniform(streams_of[10], (LEVELS, CH), jnp.float32, -0.5, 0.5), -0.5, 0.5)
    heights = place_ends(jax.random.randint(streams_of[11], (IMAGES,), SIDE4 * 7, SIDE4 * 16 + 1), jax.random.fold_in(streams_of[11], 1), SIDE4 * 7, SIDE4 * 16).astype(jnp.int32)
    widths = place_ends(jax.random.randint(streams_of[12], (IMAGES,), SIDE4 * 7, SIDE4 * 16 + 1), jax.random.fold_in(streams_of[12], 1), SIDE4 * 7, SIDE4 * 16).astype(jnp.int32)
    return {"feat4": feat4, "feat5": feat5, "feat6": feat6, "feat7": feat7, "out_grad4": out_grad4, "out_grad5": out_grad5, "out_grad6": out_grad6, "out_grad7": out_grad7, "conv_weight": conv_weight, "bn_gain": bn_gain, "bn_shift": bn_shift, "heights": heights, "widths": widths}


EPSILON = 1e-05

def level_masks(heights, widths, stride, extent):
    row_limit = (heights + stride - 1) // stride
    col_limit = (widths + stride - 1) // stride
    places = jnp.arange(extent, dtype=jnp.int32)
    inside = jnp.logical_and(places[None, :, None] < row_limit[:, None, None], places[None, None, :] < col_limit[:, None, None])
    return inside.astype(jnp.float32)

def conv_image(padded, conv_weight, extent):
    summed = jnp.zeros((extent * extent, conv_weight.shape[3]), jnp.float32)
    for tap_row in range(3):
        for tap_col in range(3):
            window = padded[tap_row:tap_row + extent, tap_col:tap_col + extent, :].reshape(extent * extent, -1)
            summed = summed + jnp.dot(window, conv_weight[tap_row, tap_col], preferred_element_type=jnp.float32)
    return summed.reshape(extent, extent, -1)

def input_grad_image(padded_back, conv_weight, extent):
    summed = jnp.zeros((extent * extent, conv_weight.shape[2]), jnp.float32)
    for tap_row in range(3):
        for tap_col in range(3):
            window = padded_back[2 - tap_row:2 - tap_row + extent, 2 - tap_col:2 - tap_col + extent, :].reshape(extent * extent, -1)
            summed = summed + lax.dot_general(window, conv_weight[tap_row, tap_col], (((1,), (1,)), ((), ())), preferred_element_type=jnp.float32)
    return summed.reshape(extent, extent, -1)

def weight_grad_image(padded, back_grad, extent):
    flat_back = back_grad.reshape(extent * extent, -1)
    tap_terms = []
    for tap_row in range(3):
        for tap_col in range(3):
            window = padded[tap_row:tap_row + extent, tap_col:tap_col + extent, :].reshape(extent * extent, -1)
            tap_terms.append(lax.dot_general(window, flat_back, (((0,), (0,)), ((), ())), preferred_element_type=jnp.float32))
    return jnp.stack(tap_terms).reshape(3, 3, padded.shape[2], flat_back.shape[1])

def reference(feat4, feat5, feat6, feat7, out_grad4, out_grad5, out_grad6, out_grad7, conv_weight, bn_gain, bn_shift, heights, widths):
    features = (feat4, feat5, feat6, feat7)
    cotangents = (out_grad4, out_grad5, out_grad6, out_grad7)
    outputs = []
    input_grads = []
    gain_rows = []
    shift_rows = []
    weight_total = jnp.zeros(conv_weight.shape, jnp.float32)
    for level_index in range(4):
        feature = features[level_index]
        extent = feature.shape[1]
        valid_mask = level_masks(heights, widths, 16 * 2 ** level_index, extent)
        weighted = valid_mask[..., None]
        masked = feature * weighted.astype(feature.dtype)
        padded = jnp.pad(masked, ((0, 0), (1, 1), (1, 1), (0, 0)))
        conv_out = lax.map(partial(conv_image, conv_weight=conv_weight, extent=extent), padded)
        pixel_count = jnp.sum(valid_mask)
        mean_value = lax.optimization_barrier(jnp.sum(conv_out * weighted, axis=(0, 1, 2))) / pixel_count
        centered = conv_out - mean_value
        variance = lax.optimization_barrier(jnp.sum(weighted * centered * centered, axis=(0, 1, 2))) / pixel_count
        inverse = lax.rsqrt(variance + EPSILON)
        normed = centered * inverse
        shifted = bn_gain[level_index] * normed + bn_shift[level_index]
        sigmoid_value = jax.nn.sigmoid(shifted)
        outputs.append((weighted * shifted * sigmoid_value).astype(jnp.bfloat16))
        slope_term = weighted * cotangents[level_index].astype(jnp.float32) * sigmoid_value * (1.0 + shifted * (1.0 - sigmoid_value))
        shift_sum = lax.optimization_barrier(jnp.sum(slope_term, axis=(0, 1, 2)))
        gain_sum = lax.optimization_barrier(jnp.sum(slope_term * normed, axis=(0, 1, 2)))
        back_grad = (weighted * (bn_gain[level_index] * inverse) * (slope_term - shift_sum / pixel_count - normed * (gain_sum / pixel_count))).astype(jnp.bfloat16)

        def add_image(carry_total, operands, extent=extent):
            return (carry_total + weight_grad_image(operands[0], operands[1], extent), None)
        weight_total, unused = lax.scan(add_image, weight_total, (padded, back_grad))
        padded_back = jnp.pad(back_grad, ((0, 0), (1, 1), (1, 1), (0, 0)))
        input_part = lax.map(partial(input_grad_image, conv_weight=conv_weight, extent=extent), padded_back)
        input_grads.append((weighted * input_part).astype(jnp.bfloat16))
        gain_rows.append(gain_sum)
        shift_rows.append(shift_sum)
    return (outputs[0], outputs[1], outputs[2], outputs[3], input_grads[0], input_grads[1], input_grads[2], input_grads[3], weight_total / IMAGES, jnp.stack(gain_rows) / IMAGES, jnp.stack(shift_rows) / IMAGES)
```

```python
import jax
import jax.numpy as jnp
from jax import lax
from jax.experimental import pallas as pl
from jax.experimental.pallas import tpu as pltpu
from jax.sharding import Mesh
from jax.sharding import PartitionSpec as P

AXES = ("wide_0", "wide_1", "group_0", "group_1")
NZ, NX, NY, NC = 8, 4, 4, 2
MESH_ID = pl.DeviceIdType.MESH
EPSILON = 1e-05
F32 = jnp.float32
BF16 = jnp.bfloat16

ROWS, COLS = 40, 32
PLACES = ((1, 0, 24), (26, 0, 12), (26, 16, 6), (26, 24, 3))
UP = (1, 25)
LOW = (26, 38)

CHUNKS = ((0, 2, 0), (2, 2, 1), (4, 2, 0), (6, 3, 1))


def kernel(
    f4, f5, f6, f7, g4, g5, g6, g7, w_hbm, gain_ref, shift_ref, h_ref, wd_ref,
    o4, o5, o6, o7, d4, d5, d6, d7, dw_hbm, dg_ref, ds_ref,
    vf4, vf5, vf6, vf7, vg4, vg5, vg6, vg7, w, wt,
    fc, gc, mask, x3, xt, conv, norm, slope, b3, res,
    sb, s0r, s1, s2,
    dw, d2r, acc1, r1, acc2, r2, acc3, zr, final,
    in_sem, st_s, st_r, c_s, c_r, out_sem,
):
    z = lax.axis_index("wide_0")
    x = lax.axis_index("wide_1")
    y = lax.axis_index("group_0")
    c = lax.axis_index("group_1")
    other = 1 - c

    barrier = pltpu.get_barrier_semaphore()

    def greet(dev):
        pl.semaphore_signal(barrier, inc=1, device_id=dev, device_id_type=MESH_ID)

    greet((z, x, y, other))
    for dx in range(NX):
        for dy in range(NY):
            if dx or dy:
                greet((z, (x + dx) % NX, (y + dy) % NY, c))
    for dz in range(1, NZ):
        for dc in range(NC):
            greet(((z + dz) % NZ, x, y, (c + dc) % NC))

    loads = []
    for i, (src, dst) in enumerate(
        ((f4, vf4), (f5, vf5), (f6, vf6), (f7, vf7), (w_hbm, w),
         (g4, vg4), (g5, vg5), (g6, vg6), (g7, vg7))
    ):
        copy = pltpu.make_async_copy(src, dst, in_sem.at[i])
        copy.start()
        loads.append(copy)

    def rows_at(r):
        return pl.ds(pl.multiple_of(r * COLS, COLS), COLS)

    limits = []
    for k in range(4):
        stride = 16 * 2**k
        limits.append(((h_ref[0] + stride - 1) // stride, (wd_ref[0] + stride - 1) // stride))
    col = lax.broadcasted_iota(jnp.int32, (COLS, 256), 0)

    def clear_row(r, carry):
        fc[r] = jnp.zeros((COLS, 256), F32)
        gc[r] = jnp.zeros((COLS, 256), F32)
        mask[rows_at(r)] = jnp.zeros((COLS, 256), F32)
        return carry

    lax.fori_loop(0, ROWS, clear_row, 0)

    def clear_b3(r, carry):
        b3[rows_at(r)] = jnp.zeros((COLS, 768), BF16)
        return carry

    lax.fori_loop(0, ROWS + 2, clear_b3, 0)

    def mask_up(r, carry):
        inside = jnp.logical_and(
            r - UP[0] < jnp.minimum(limits[0][0], 24), col < jnp.minimum(limits[0][1], 24)
        )
        mask[rows_at(r)] = jnp.where(inside, 1.0, 0.0)
        return carry

    lax.fori_loop(UP[0], UP[1], mask_up, 0)

    def mask_low(r, carry):
        inside = None
        for k in (1, 2, 3):
            _, first, side = PLACES[k]
            here = jnp.logical_and(
                r - LOW[0] < jnp.minimum(limits[k][0], side),
                jnp.logical_and(
                    col >= first, col - first < jnp.minimum(limits[k][1], side)
                ),
            )
            inside = here if inside is None else jnp.logical_or(inside, here)
        mask[rows_at(r)] = jnp.where(inside, 1.0, 0.0)
        return carry

    lax.fori_loop(LOW[0], LOW[1], mask_low, 0)

    for k, ref in enumerate((vf4, vf5, vf6, vf7)):
        loads[k].wait()
        first_row, first, side = PLACES[k]
        fc[first_row : first_row + side, first : first + side, :] = ref[0].astype(F32)

    def spread(r, carry):
        value = fc[r] * mask[rows_at(r)]
        at = rows_at(r)
        x3[at, 0:256] = pltpu.roll(value, 1, 0).astype(BF16)
        x3[at, 256:512] = value.astype(BF16)
        x3[at, 512:768] = pltpu.roll(value, COLS - 1, 0).astype(BF16)
        return carry

    lax.fori_loop(0, ROWS, spread, 0)
    loads[4].wait()

    flat = (LOW[1] - 1) * COLS
    total = None
    for a in range(3):
        part = jnp.dot(
            x3[a * COLS : a * COLS + flat, :],
            w[a * 768 : (a + 1) * 768, :],
            preferred_element_type=F32,
        )
        total = part if total is None else total + part
    conv[COLS : COLS + flat, :] = total

    zero = jnp.zeros((COLS, 256), F32)

    def down(value):
        return jnp.sum(value, axis=0, keepdims=True)

    def by_level(up, low):
        out = [down(up)]
        for k in (1, 2, 3):
            _, first, side = PLACES[k]
            out.append(down(jnp.where(jnp.logical_and(col >= first, col < first + 8 * (1 if k > 1 else 2)), low, 0.0)))
        return out

    def moments(r, carry):
        s, q, n = carry
        m = mask[rows_at(r)]
        v = conv[rows_at(r)]
        mv = m * v
        return s + mv, q + mv * v, n + m

    up = lax.fori_loop(UP[0], UP[1], moments, (zero, zero, zero))
    low = lax.fori_loop(LOW[0], LOW[1], moments, (zero, zero, zero))
    sums = by_level(up[0], low[0])
    squares = by_level(up[1], low[1])
    tallies = by_level(up[2], low[2])
    lane = lax.broadcasted_iota(jnp.int32, (1, 256), 1)
    counts_row = jnp.zeros((1, 256), F32)
    for k in range(4):
        counts_row = jnp.where(lane // 64 == k, tallies[k], counts_row)

    def remote(src, dst, send, recv, dev):
        return pltpu.make_async_remote_copy(
            src_ref=src, dst_ref=dst, send_sem=send, recv_sem=recv,
            device_id=dev, device_id_type=MESH_ID,
        )

    pl.semaphore_wait(barrier, 30)

    def stats(which, halves, filler_a=None, filler_b=None):
        for half in range(2):
            for i, row in enumerate(halves[half]):
                sb[which, half, i] = row
        first = remote(
            sb.at[which, other], s0r.at[which], st_s.at[which, 0], st_r.at[which, 0],
            (z, x, y, other),
        )
        first.start()
        first.wait()
        own = x * NY + y
        s1[which, own] = sb[which, c] + s0r[which]
        plane = []
        for dx in range(NX):
            for dy in range(NY):
                if dx or dy:
                    slot = 1 + dx * NY + dy
                    plane.append(remote(
                        s1.at[which, own], s1.at[which, own],
                        st_s.at[which, slot], st_r.at[which, slot],
                        (z, (x + dx) % NX, (y + dy) % NY, c),
                    ))
        for copy in plane:
            copy.start()
        if filler_a is not None:
            filler_a()
        for copy in plane:
            copy.wait()
        value = s1[which, 0]
        for i in range(1, NX * NY):
            value = value + s1[which, i]
        s2[which, c, z] = value
        column = []
        for dz in range(NZ):
            for dc in range(NC):
                if dz or dc:
                    slot = 17 + dz * NC + dc
                    column.append(remote(
                        s2.at[which, c, z], s2.at[which, c, z],
                        st_s.at[which, slot], st_r.at[which, slot],
                        ((z + dz) % NZ, x, y, (c + dc) % NC),
                    ))
        for copy in column:
            copy.start()
        if filler_b is not None:
            filler_b()
        for copy in column:
            copy.wait()
        outs = []
        for half in range(2):
            value = s2[which, half, 0]
            for i in range(1, NZ):
                value = value + s2[which, half, i]
            outs.append([value[i] for i in range(5)])
        return outs

    def fill_transposes():
        def turn(b, carry):
            at = pl.ds(pl.multiple_of(b * 256, 256), 256)
            xt[at, :] = x3[:, at].T
            return carry

        for b in range(3):
            xt[b * 256 : (b + 1) * 256, :] = x3[:, b * 256 : (b + 1) * 256].T

    def fill_weights():
        def turn(t, carry):
            at = pl.ds(pl.multiple_of(t * 256, 256), 256)
            wt[at, :] = w[at, :].T
            return carry

        lax.fori_loop(0, 9, turn, 0)
        for k, ref in enumerate((vg4, vg5, vg6, vg7)):
            loads[5 + k].wait()
            first_row, first, side = PLACES[k]
            gc[first_row : first_row + side, first : first + side, :] = ref[0].astype(F32)

    (sum_rows, square_rows) = stats(
        0, (sums + [counts_row], squares + [counts_row]), fill_transposes, fill_weights
    )
    means, inverses, counts = [], [], []
    for k in range(4):
        n = down(jnp.where(lane == 64 * k, sum_rows[4], 0.0).T).T if False else jnp.sum(
            jnp.where(lane == 64 * k, sum_rows[4], 0.0), axis=1, keepdims=True
        )
        n = jnp.broadcast_to(n, (1, 256))
        mean = sum_rows[k] / n
        counts.append(n)
        means.append(mean)
        inverses.append(lax.rsqrt(square_rows[k] / n - mean * mean + EPSILON))
    gains = [gain_ref[k : k + 1, :] for k in range(4)]
    shifts = [shift_ref[k : k + 1, :] for k in range(4)]

    def low_of(rows):
        return jnp.where(col < 16, rows[1], jnp.where(col < 24, rows[2], rows[3]))

    def activate(params):
        mean, inverse, gain, shift = params

        def step(r, carry):
            s, g = carry
            at = rows_at(r)
            m = mask[at]
            normed = (conv[at] - mean) * inverse
            shifted = gain * normed + shift
            sig = jax.nn.sigmoid(shifted)
            res[r] = m * shifted * sig
            slope_value = m * gc[r] * sig * (1.0 + shifted * (1.0 - sig))
            norm[at] = normed
            slope[at] = slope_value
            return s + slope_value, g + slope_value * normed

        return step

    up_params = (means[0], inverses[0], gains[0], shifts[0])
    low_params = (low_of(means), low_of(inverses), low_of(gains), low_of(shifts))
    up = lax.fori_loop(UP[0], UP[1], activate(up_params), (zero, zero))
    low = lax.fori_loop(LOW[0], LOW[1], activate(low_params), (zero, zero))
    shift_local = by_level(up[0], low[0])
    gain_local = by_level(up[1], low[1])

    def take_out(refs):
        for k, ref in enumerate(refs):
            first_row, first, side = PLACES[k]
            ref[0] = res[first_row : first_row + side, first : first + side, :].astype(BF16)

    (shift_rows, gain_rows) = stats(
        1, (shift_local + [counts_row], gain_local + [counts_row]),
        lambda: take_out((o4, o5, o6, o7)),
    )
    for k in range(4):
        dg_ref[k : k + 1, :] = gain_rows[k] * (1.0 / 256.0)
        ds_ref[k : k + 1, :] = shift_rows[k] * (1.0 / 256.0)

    def back(params):
        scale, base, lean = params

        def step(r, carry):
            at = rows_at(r)
            value = mask[at] * scale * (slope[at] - base - norm[at] * lean)
            value = value.astype(BF16).astype(F32)
            to = rows_at(r + 1)
            b3[to, 0:256] = pltpu.roll(value, COLS - 1, 0).astype(BF16)
            b3[to, 256:512] = value.astype(BF16)
            b3[to, 512:768] = pltpu.roll(value, 1, 0).astype(BF16)
            return carry

        return step

    scales = [gains[k] * inverses[k] for k in range(4)]
    bases = [shift_rows[k] / counts[k] for k in range(4)]
    leans = [gain_rows[k] / counts[k] for k in range(4)]
    lax.fori_loop(UP[0], UP[1], back((scales[0], bases[0], leans[0])), 0)
    lax.fori_loop(LOW[0], LOW[1], back((low_of(scales), low_of(bases), low_of(leans))), 0)

    def ring(axis, d):
        if axis == 0:
            return (z, (x + d) % NX, y, c)
        return (z, x, (y + d) % NY, c)

    def place(axis):
        return x if axis == 0 else y

    def shifted_place(axis, d):
        return (place(axis) + d) % 4

    def al(value, unit):
        return pl.multiple_of(value, unit)

    pending = {}

    def start(key, copies):
        for copy in copies:
            copy.start()
        pending[key] = copies

    def finish(key):
        for copy in pending.pop(key):
            copy.wait()

    def sems(i, slot):
        return c_s.at[i, slot], c_r.at[i, slot]

    def stage0(i):
        t0, nt, axis = CHUNKS[i]
        for t in range(t0, t0 + nt):
            a, b = divmod(t, 3)
            dw[t] = jnp.dot(
                xt[b * 256 : (b + 1) * 256, :],
                b3[(2 - a) * COLS : (2 - a) * COLS + ROWS * COLS, 256:512],
                preferred_element_type=F32,
            )
        start((0, i), [remote(
            dw.at[pl.ds(t0, nt), pl.ds(al(other * 128, 128), 128), :],
            d2r.at[pl.ds(t0, nt)], *sems(i, 0), (z, x, y, other),
        )])

    def stage1(i):
        t0, nt, axis = CHUNKS[i]
        finish((0, i))
        for t in range(t0, t0 + nt):
            acc1[t] = dw[t, pl.ds(al(c * 128, 128), 128), :] + d2r[t]
        start((1, i), [remote(
            acc1.at[pl.ds(t0, nt), pl.ds(al(shifted_place(axis, d) * 32, 32), 32), :],
            r1.at[d - 1, pl.ds(t0, nt)], *sems(i, d), ring(axis, d),
        ) for d in (1, 2, 3)])

    def stage2(i):
        t0, nt, axis = CHUNKS[i]
        second = 1 - axis
        finish((1, i))
        for t in range(t0, t0 + nt):
            own = acc1[t, pl.ds(al(place(axis) * 32, 32), 32), :]
            acc2[t] = own + r1[0, t] + r1[1, t] + r1[2, t]
        start((2, i), [remote(
            acc2.at[pl.ds(t0, nt), pl.ds(al(shifted_place(second, d) * 8, 8), 8), :],
            r2.at[d - 1, pl.ds(t0, nt)], *sems(i, 3 + d), ring(second, d),
        ) for d in (1, 2, 3)])

    def stage3(i):
        t0, nt, axis = CHUNKS[i]
        second = 1 - axis
        finish((2, i))
        for t in range(t0, t0 + nt):
            own = acc2[t, pl.ds(al(place(second) * 8, 8), 8), :]
            acc3[t] = own + r2[0, t] + r2[1, t] + r2[2, t]
        start((3, i), [remote(
            acc3.at[pl.ds(t0, nt), pl.ds((z + d) % NZ, 1), :],
            zr.at[pl.ds(t0, nt), pl.ds(z, 1), :], *sems(i, 6 + d), ((z + d) % NZ, x, y, c),
        ) for d in range(1, NZ)])
        for t in range(t0, t0 + nt):
            zr[t, pl.ds(z, 1), :] = acc3[t, pl.ds(z, 1), :]

    def home(axis):
        return c * 128 + place(axis) * 32

    def stage4(i):
        t0, nt, axis = CHUNKS[i]
        second = 1 - axis
        finish((3, i))
        row = home(axis) + place(second) * 8 + z
        for t in range(t0, t0 + nt):
            final[t, pl.ds(row, 1), :] = jnp.sum(zr[t], axis=0, keepdims=True) * (1.0 / 256.0)
        here = final.at[pl.ds(t0, nt), pl.ds(row, 1), :]
        start((4, i), [remote(
            here, here, *sems(i, 13 + d), ((z + d) % NZ, x, y, c),
        ) for d in range(1, NZ)])

    def stage5(i):
        t0, nt, axis = CHUNKS[i]
        second = 1 - axis
        finish((4, i))
        here = final.at[pl.ds(t0, nt), pl.ds(al(home(axis) + place(second) * 8, 8), 8), :]
        start((5, i), [remote(
            here, here, *sems(i, 20 + d), ring(second, d),
        ) for d in (1, 2, 3)])

    def stage6(i):
        t0, nt, axis = CHUNKS[i]
        finish((5, i))
        here = final.at[pl.ds(t0, nt), pl.ds(al(home(axis), 32), 32), :]
        start((6, i), [remote(
            here, here, *sems(i, 23 + d), ring(axis, d),
        ) for d in (1, 2, 3)])

    def stage7(i):
        t0, nt, axis = CHUNKS[i]
        finish((6, i))
        here = final.at[pl.ds(t0, nt), pl.ds(al(c * 128, 128), 128), :]
        start((7, i), [remote(here, here, *sems(i, 27), (z, x, y, other))])

    def stage8(i):
        t0, nt, axis = CHUNKS[i]
        finish((7, i))
        copy = pltpu.make_async_copy(
            final.at[pl.ds(t0, nt)], dw_hbm.at[pl.ds(t0, nt)], out_sem.at[i]
        )
        copy.start()
        pending[(8, i)] = [copy]

    stages = (stage0, stage1, stage2, stage3, stage4, stage5, stage6, stage7, stage8)
    count = len(CHUNKS)

    for i in range(count):
        stage0(i)
        if i:
            stage1(i - 1)
    stage1(count - 1)

    total = None
    for a in range(3):
        part = jnp.dot(
            b3[(3 - a) * COLS : (3 - a) * COLS + flat, :],
            wt[a * 768 : (a + 1) * 768, :],
            preferred_element_type=F32,
        )
        total = part if total is None else total + part
    conv[COLS : COLS + flat, :] = total

    def masked(r, carry):
        res[r] = conv[rows_at(r)] * mask[rows_at(r)]
        return carry

    lax.fori_loop(1, LOW[1], masked, 0)
    take_out((d4, d5, d6, d7))

    for step in range(2, 9 + count - 1):
        for i in range(count):
            s = step - i
            if 2 <= s <= 8:
                stages[s](i)
    for i in range(count):
        finish((8, i))


def shards(*args):
    (f4, f5, f6, f7, g4, g5, g6, g7, conv_weight, gain, shift, heights, widths) = args
    any_spec = pl.BlockSpec(memory_space=pl.ANY)
    vmem_spec = pl.BlockSpec(memory_space=pltpu.VMEM)
    smem_spec = pl.BlockSpec(memory_space=pltpu.SMEM)
    feats = (f4, f5, f6, f7)
    image_shapes = [jax.ShapeDtypeStruct(f.shape, BF16) for f in feats]
    vm = pltpu.VMEM
    scratch = (
        [vm(f.shape, BF16) for f in feats]
        + [vm(f.shape, BF16) for f in feats]
        + [
            vm((2304, 256), BF16),
            vm((2304, 256), BF16),
            vm((ROWS, COLS, 256), F32),
            vm((ROWS, COLS, 256), F32),
            vm((ROWS * COLS, 256), F32),
            vm((ROWS * COLS, 768), BF16),
            vm((768, ROWS * COLS), BF16),
            vm((ROWS * COLS, 256), F32),
            vm((ROWS * COLS, 256), F32),
            vm((ROWS * COLS, 256), F32),
            vm(((ROWS + 2) * COLS, 768), BF16),
            vm((ROWS, COLS, 256), F32),
            vm((2, 2, 5, 1, 256), F32),
            vm((2, 5, 1, 256), F32),
            vm((2, 16, 5, 1, 256), F32),
            vm((2, 2, 8, 5, 1, 256), F32),
            vm((9, 256, 256), F32),
            vm((9, 128, 256), F32),
            vm((9, 128, 256), F32),
            vm((3, 9, 32, 256), F32),
            vm((9, 32, 256), F32),
            vm((3, 9, 8, 256), F32),
            vm((9, 8, 256), F32),
            vm((9, 8, 256), F32),
            vm((9, 256, 256), F32),
            pltpu.SemaphoreType.DMA((9,)),
            pltpu.SemaphoreType.DMA((2, 33)),
            pltpu.SemaphoreType.DMA((2, 33)),
            pltpu.SemaphoreType.DMA((len(CHUNKS), 28)),
            pltpu.SemaphoreType.DMA((len(CHUNKS), 28)),
            pltpu.SemaphoreType.DMA((len(CHUNKS),)),
        ]
    )
    small = jax.ShapeDtypeStruct((4, 256), F32)
    outs = pl.pallas_call(
        kernel,
        out_shape=image_shapes + image_shapes + [jax.ShapeDtypeStruct((9, 256, 256), F32), small, small],
        in_specs=[any_spec] * 9 + [vmem_spec] * 2 + [smem_spec] * 2,
        out_specs=[vmem_spec] * 8 + [any_spec] + [vmem_spec] * 2,
        scratch_shapes=scratch,
        compiler_params=pltpu.CompilerParams(
            collective_id=0, has_side_effects=True, vmem_limit_bytes=60 * 1024 * 1024
        ),
        name="fused_step",
    )(f4, f5, f6, f7, g4, g5, g6, g7, conv_weight.reshape(2304, 256), gain, shift, heights, widths)
    outs = list(outs)
    outs[8] = outs[8].reshape(3, 3, 256, 256)
    return tuple(outs)


def solution(mesh):
    torus = Mesh(mesh.devices.reshape(NZ, NX, NY, NC), AXES)
    image = P(AXES, None, None, None)
    in_specs = (image,) * 8 + (P(), P(), P(), P(AXES), P(AXES))
    out_specs = (image,) * 8 + (P(), P(), P())
    return jax.shard_map(shards, mesh=torus, in_specs=in_specs, out_specs=out_specs, check_vma=False)
```

```python
import jax
import jax.numpy as jnp
from jax import lax
from jax.experimental import pallas as pl
from jax.experimental.pallas import tpu as pltpu
from jax.sharding import Mesh
from jax.sharding import PartitionSpec as P

AXES = ("wide_0", "wide_1", "group_0", "group_1")
NZ, NX, NY, NC = 8, 4, 4, 2
MESH_ID = pl.DeviceIdType.MESH
EPSILON = 1e-05
F32 = jnp.float32
BF16 = jnp.bfloat16

ROWS, COLS = 40, 32
PLACES = ((1, 0, 24), (26, 0, 12), (26, 16, 6), (26, 24, 3))
UP = (1, 25)
LOW = (26, 38)

FUSED_VMEM = 63_780_000

CHUNKS = ((0, 2, 0), (2, 2, 1), (4, 2, 0), (6, 3, 1))


def kernel(
    f4, f5, f6, f7, g4, g5, g6, g7, w_hbm, gain_hbm, shift_hbm, size_hbm,
    o4, o5, o6, o7, d4, d5, d6, d7, final, dg_ref, ds_ref,
    gain_ref, shift_ref, size_ref,
    vf4, vf5, vf6, vf7, vg4, vg5, vg6, vg7, w, wt,
    fc, gc, mask, x3, xt, conv, norm, slope, b3, res,
    sb, s0r, s1, s2,
    dw, d2r, acc1, r1, acc2, r2, zs, zr, zg,
    in_sem, st_s, st_r, c_s, c_r,
):
    z = lax.axis_index("wide_0")
    x = lax.axis_index("wide_1")
    y = lax.axis_index("group_0")
    c = lax.axis_index("group_1")
    other = 1 - c

    barrier = pltpu.get_barrier_semaphore()

    def greet(dev):
        pl.semaphore_signal(barrier, inc=1, device_id=dev, device_id_type=MESH_ID)

    greet((z, x, y, other))
    for dx in range(NX):
        for dy in range(NY):
            if dx or dy:
                greet((z, (x + dx) % NX, (y + dy) % NY, c))
    for dz in range(1, NZ):
        for dc in range(NC):
            greet(((z + dz) % NZ, x, y, (c + dc) % NC))

    loads = []
    for i, (src, dst) in enumerate(
        ((f4, vf4), (f5, vf5), (f6, vf6), (f7, vf7), (w_hbm, w),
         (g4, vg4), (g5, vg5), (g6, vg6), (g7, vg7),
         (gain_hbm, gain_ref), (shift_hbm, shift_ref), (size_hbm, size_ref))
    ):
        copy = pltpu.make_async_copy(src, dst, in_sem.at[i])
        copy.start()
        loads.append(copy)

    def rows_at(r):
        return pl.ds(pl.multiple_of(r * COLS, COLS), COLS)

    col = lax.broadcasted_iota(jnp.int32, (COLS, 256), 0)

    def clear_row(r, carry):
        fc[r] = jnp.zeros((COLS, 256), F32)
        gc[r] = jnp.zeros((COLS, 256), F32)
        mask[rows_at(r)] = jnp.zeros((COLS, 256), F32)
        return carry

    lax.fori_loop(0, ROWS, clear_row, 0)

    def clear_b3(r, carry):
        b3[rows_at(r)] = jnp.zeros((COLS, 768), BF16)
        return carry

    lax.fori_loop(0, ROWS + 2, clear_b3, 0)

    loads[11].wait()
    limits = []
    for k in range(4):
        stride = 16 * 2**k
        limits.append([
            jnp.broadcast_to(
                lax.shift_right_arithmetic(
                    size_ref[i : i + 1, :] + (stride - 1), jnp.full((1, 256), 4 + k, jnp.int32)
                ),
                (COLS, 256),
            )
            for i in range(2)
        ])

    def mask_up(r, carry):
        inside = jnp.logical_and(
            r - UP[0] < jnp.minimum(limits[0][0], 24), col < jnp.minimum(limits[0][1], 24)
        )
        mask[rows_at(r)] = jnp.where(inside, 1.0, 0.0)
        return carry

    lax.fori_loop(UP[0], UP[1], mask_up, 0)

    def mask_low(r, carry):
        inside = None
        for k in (1, 2, 3):
            _, first, side = PLACES[k]
            here = jnp.logical_and(
                r - LOW[0] < jnp.minimum(limits[k][0], side),
                jnp.logical_and(
                    col >= first, col - first < jnp.minimum(limits[k][1], side)
                ),
            )
            inside = here if inside is None else jnp.logical_or(inside, here)
        mask[rows_at(r)] = jnp.where(inside, 1.0, 0.0)
        return carry

    lax.fori_loop(LOW[0], LOW[1], mask_low, 0)

    for k, ref in enumerate((vf4, vf5, vf6, vf7)):
        loads[k].wait()
        first_row, first, side = PLACES[k]
        fc[first_row : first_row + side, first : first + side, :] = ref[0].astype(F32)

    def spread(r, carry):
        value = fc[r] * mask[rows_at(r)]
        at = rows_at(r)
        x3[at, 0:256] = pltpu.roll(value, 1, 0).astype(BF16)
        x3[at, 256:512] = value.astype(BF16)
        x3[at, 512:768] = pltpu.roll(value, COLS - 1, 0).astype(BF16)
        return carry

    lax.fori_loop(0, ROWS, spread, 0)
    loads[4].wait()

    flat = (LOW[1] - 1) * COLS
    total = None
    for a in range(3):
        part = jnp.dot(
            x3[a * COLS : a * COLS + flat, :],
            w[a * 768 : (a + 1) * 768, :],
            preferred_element_type=F32,
        )
        total = part if total is None else total + part
    conv[COLS : COLS + flat, :] = total

    zero = jnp.zeros((COLS, 256), F32)

    def down(value):
        return jnp.sum(value, axis=0, keepdims=True)

    def by_level(up, low):
        out = [down(up)]
        for k in (1, 2, 3):
            _, first, side = PLACES[k]
            out.append(down(jnp.where(jnp.logical_and(col >= first, col < first + 8 * (1 if k > 1 else 2)), low, 0.0)))
        return out

    def moments(r, carry):
        s, q, n = carry
        m = mask[rows_at(r)]
        v = conv[rows_at(r)]
        mv = m * v
        return s + mv, q + mv * v, n + m

    up = lax.fori_loop(UP[0], UP[1], moments, (zero, zero, zero))
    low = lax.fori_loop(LOW[0], LOW[1], moments, (zero, zero, zero))
    sums = by_level(up[0], low[0])
    squares = by_level(up[1], low[1])
    tallies = by_level(up[2], low[2])
    lane = lax.broadcasted_iota(jnp.int32, (1, 256), 1)
    counts_row = jnp.zeros((1, 256), F32)
    for k in range(4):
        counts_row = jnp.where(lane // 64 == k, tallies[k], counts_row)

    def remote(src, dst, send, recv, dev):
        return pltpu.make_async_remote_copy(
            src_ref=src, dst_ref=dst, send_sem=send, recv_sem=recv,
            device_id=dev, device_id_type=MESH_ID,
        )

    pl.semaphore_wait(barrier, 30)

    def stats(which, halves, filler_a=None, filler_b=None):
        for half in range(2):
            for i, row in enumerate(halves[half]):
                sb[which, half, i] = row
        first = remote(
            sb.at[which, other], s0r.at[which], st_s.at[which, 0], st_r.at[which, 0],
            (z, x, y, other),
        )
        first.start()
        first.wait()
        own = x * NY + y
        s1[which, own] = sb[which, c] + s0r[which]
        plane = []
        for dx in range(NX):
            for dy in range(NY):
                if dx or dy:
                    slot = 1 + dx * NY + dy
                    plane.append(remote(
                        s1.at[which, own], s1.at[which, own],
                        st_s.at[which, slot], st_r.at[which, slot],
                        (z, (x + dx) % NX, (y + dy) % NY, c),
                    ))
        for copy in plane:
            copy.start()
        if filler_a is not None:
            filler_a()
        for copy in plane:
            copy.wait()
        value = s1[which, 0]
        for i in range(1, NX * NY):
            value = value + s1[which, i]
        s2[which, c, z] = value
        column = []
        for dz in range(NZ):
            for dc in range(NC):
                if dz or dc:
                    slot = 17 + dz * NC + dc
                    column.append(remote(
                        s2.at[which, c, z], s2.at[which, c, z],
                        st_s.at[which, slot], st_r.at[which, slot],
                        ((z + dz) % NZ, x, y, (c + dc) % NC),
                    ))
        for copy in column:
            copy.start()
        if filler_b is not None:
            filler_b()
        for copy in column:
            copy.wait()
        outs = []
        for half in range(2):
            value = s2[which, half, 0]
            for i in range(1, NZ):
                value = value + s2[which, half, i]
            outs.append([value[i] for i in range(5)])
        return outs

    def fill_transposes():
        for b in range(3):
            xt[b * 256 : (b + 1) * 256, :] = x3[:, b * 256 : (b + 1) * 256].T

    def fill_weights():
        def turn(t, carry):
            at = pl.ds(pl.multiple_of(t * 256, 256), 256)
            wt[at, :] = w[at, :].T
            return carry

        lax.fori_loop(0, 9, turn, 0)
        for k, ref in enumerate((vg4, vg5, vg6, vg7)):
            loads[5 + k].wait()
            first_row, first, side = PLACES[k]
            gc[first_row : first_row + side, first : first + side, :] = ref[0].astype(F32)

    (sum_rows, square_rows) = stats(
        0, (sums + [counts_row], squares + [counts_row]), fill_transposes, fill_weights
    )
    means, inverses, counts = [], [], []
    for k in range(4):
        n = jnp.sum(jnp.where(lane == 64 * k, sum_rows[4], 0.0), axis=1, keepdims=True)
        n = jnp.broadcast_to(n, (1, 256))
        mean = sum_rows[k] / n
        counts.append(n)
        means.append(mean)
        inverses.append(lax.rsqrt(square_rows[k] / n - mean * mean + EPSILON))
    loads[9].wait()
    loads[10].wait()
    gains = [gain_ref[k : k + 1, :] for k in range(4)]
    shifts = [shift_ref[k : k + 1, :] for k in range(4)]

    def low_of(rows):
        return jnp.where(col < 16, rows[1], jnp.where(col < 24, rows[2], rows[3]))

    def activate(params):
        mean, inverse, gain, shift = params

        def step(r, carry):
            s, g = carry
            at = rows_at(r)
            m = mask[at]
            normed = (conv[at] - mean) * inverse
            shifted = gain * normed + shift
            sig = jax.nn.sigmoid(shifted)
            res[r] = m * shifted * sig
            slope_value = m * gc[r] * sig * (1.0 + shifted * (1.0 - sig))
            norm[at] = normed
            slope[at] = slope_value
            return s + slope_value, g + slope_value * normed

        return step

    up_params = (means[0], inverses[0], gains[0], shifts[0])
    low_params = (low_of(means), low_of(inverses), low_of(gains), low_of(shifts))
    up = lax.fori_loop(UP[0], UP[1], activate(up_params), (zero, zero))
    low = lax.fori_loop(LOW[0], LOW[1], activate(low_params), (zero, zero))
    shift_local = by_level(up[0], low[0])
    gain_local = by_level(up[1], low[1])

    def take_out(refs):
        for k, ref in enumerate(refs):
            first_row, first, side = PLACES[k]
            ref[0] = res[first_row : first_row + side, first : first + side, :].astype(BF16)

    (shift_rows, gain_rows) = stats(
        1, (shift_local + [counts_row], gain_local + [counts_row]),
        lambda: take_out((o4, o5, o6, o7)),
    )
    for k in range(4):
        dg_ref[k : k + 1, :] = gain_rows[k] * (1.0 / 256.0)
        ds_ref[k : k + 1, :] = shift_rows[k] * (1.0 / 256.0)

    def back(params):
        scale, base, lean = params

        def step(r, carry):
            at = rows_at(r)
            value = mask[at] * scale * (slope[at] - base - norm[at] * lean)
            value = value.astype(BF16).astype(F32)
            to = rows_at(r + 1)
            b3[to, 0:256] = pltpu.roll(value, COLS - 1, 0).astype(BF16)
            b3[to, 256:512] = value.astype(BF16)
            b3[to, 512:768] = pltpu.roll(value, 1, 0).astype(BF16)
            return carry

        return step

    scales = [gains[k] * inverses[k] for k in range(4)]
    bases = [shift_rows[k] / counts[k] for k in range(4)]
    leans = [gain_rows[k] / counts[k] for k in range(4)]
    lax.fori_loop(UP[0], UP[1], back((scales[0], bases[0], leans[0])), 0)
    lax.fori_loop(LOW[0], LOW[1], back((low_of(scales), low_of(bases), low_of(leans))), 0)

    def ring(axis, d):
        if axis == 0:
            return (z, (x + d) % NX, y, c)
        return (z, x, (y + d) % NY, c)

    def place(axis):
        return x if axis == 0 else y

    def shifted_place(axis, d):
        return (place(axis) + d) % 4

    def al(value, unit):
        return pl.multiple_of(value, unit)

    pending = {}

    def start(key, copies):
        for copy in copies:
            copy.start()
        pending[key] = copies

    def finish(key):
        for copy in pending.pop(key):
            copy.wait()

    def sems(i, slot):
        return c_s.at[i, slot], c_r.at[i, slot]

    def stage0(i):
        t0, nt, axis = CHUNKS[i]
        for t in range(t0, t0 + nt):
            a, b = divmod(t, 3)
            dw[t] = jnp.dot(
                xt[b * 256 : (b + 1) * 256, :],
                b3[(2 - a) * COLS : (2 - a) * COLS + ROWS * COLS, 256:512],
                preferred_element_type=F32,
            )
        start((0, i), [remote(
            dw.at[pl.ds(t0, nt), pl.ds(al(other * 128, 128), 128), :],
            d2r.at[pl.ds(t0, nt)], *sems(i, 0), (z, x, y, other),
        )])

    def stage1(i):
        t0, nt, axis = CHUNKS[i]
        finish((0, i))
        for t in range(t0, t0 + nt):
            acc1[t] = dw[t, pl.ds(al(c * 128, 128), 128), :] + d2r[t]
        start((1, i), [remote(
            acc1.at[pl.ds(t0, nt), pl.ds(al(shifted_place(axis, d) * 32, 32), 32), :],
            r1.at[d - 1, pl.ds(t0, nt)], *sems(i, d), ring(axis, d),
        ) for d in (1, 2, 3)])

    def stage2(i):
        t0, nt, axis = CHUNKS[i]
        second = 1 - axis
        finish((1, i))
        for t in range(t0, t0 + nt):
            own = acc1[t, pl.ds(al(place(axis) * 32, 32), 32), :]
            acc2[t] = own + r1[0, t] + r1[1, t] + r1[2, t]
        start((2, i), [remote(
            acc2.at[pl.ds(t0, nt), pl.ds(al(shifted_place(second, d) * 8, 8), 8), :],
            r2.at[d - 1, pl.ds(t0, nt)], *sems(i, 3 + d), ring(second, d),
        ) for d in (1, 2, 3)])

    def stage3(i):
        t0, nt, axis = CHUNKS[i]
        second = 1 - axis
        finish((2, i))
        for t in range(t0, t0 + nt):
            own = acc2[t, pl.ds(al(place(second) * 8, 8), 8), :]
            value = own + r2[0, t] + r2[1, t] + r2[2, t]
            for j in range(NZ):
                zs[j, t] = value[j : j + 1, :]
        start((3, i), [remote(
            zs.at[(z + d) % NZ, pl.ds(t0, nt)], zr.at[d - 1, pl.ds(t0, nt)],
            *sems(i, 6 + d), ((z + d) % NZ, x, y, c),
        ) for d in range(1, NZ)])

    def home(axis):
        return c * 128 + place(axis) * 32

    def stage4(i):
        t0, nt, axis = CHUNKS[i]
        finish((3, i))
        for t in range(t0, t0 + nt):
            value = zs[z, t]
            for d in range(1, NZ):
                value = value + zr[d - 1, t]
            zg[z, t] = value * (1.0 / 256.0)
        here = zg.at[z, pl.ds(t0, nt)]
        start((4, i), [remote(
            here, here, *sems(i, 13 + d), ((z + d) % NZ, x, y, c),
        ) for d in range(1, NZ)])

    def stage5(i):
        t0, nt, axis = CHUNKS[i]
        second = 1 - axis
        finish((4, i))
        base = home(axis) + place(second) * 8
        for t in range(t0, t0 + nt):
            rows = [zg[j, t] for j in range(NZ)]
            final[t, pl.ds(al(base, 8), 8), :] = jnp.concatenate(rows, axis=0)
        here = final.at[pl.ds(t0, nt), pl.ds(al(home(axis) + place(second) * 8, 8), 8), :]
        start((5, i), [remote(
            here, here, *sems(i, 20 + d), ring(second, d),
        ) for d in (1, 2, 3)])

    def stage6(i):
        t0, nt, axis = CHUNKS[i]
        finish((5, i))
        here = final.at[pl.ds(t0, nt), pl.ds(al(home(axis), 32), 32), :]
        start((6, i), [remote(
            here, here, *sems(i, 23 + d), ring(axis, d),
        ) for d in (1, 2, 3)])

    def stage7(i):
        t0, nt, axis = CHUNKS[i]
        finish((6, i))
        here = final.at[pl.ds(t0, nt), pl.ds(al(c * 128, 128), 128), :]
        start((7, i), [remote(here, here, *sems(i, 27), (z, x, y, other))])

    stages = (stage0, stage1, stage2, stage3, stage4, stage5, stage6, stage7)
    count = len(CHUNKS)

    for i in range(count):
        stage0(i)
        if i:
            stage1(i - 1)
    stage1(count - 1)

    total = None
    for a in range(3):
        part = jnp.dot(
            b3[(3 - a) * COLS : (3 - a) * COLS + flat, :],
            wt[a * 768 : (a + 1) * 768, :],
            preferred_element_type=F32,
        )
        total = part if total is None else total + part
    conv[COLS : COLS + flat, :] = total

    def masked(r, carry):
        res[r] = conv[rows_at(r)] * mask[rows_at(r)]
        return carry

    lax.fori_loop(1, LOW[1], masked, 0)
    take_out((d4, d5, d6, d7))

    for step in range(2, 8 + count - 1):
        for i in range(count):
            s = step - i
            if 2 <= s <= 7:
                stages[s](i)
    for i in range(count):
        finish((7, i))


def write_out(*refs):
    count = len(refs) // 2
    sem = refs[-1]
    copies = [pltpu.make_async_copy(refs[i], refs[count + i], sem.at[i]) for i in range(count)]
    for copy in copies:
        copy.start()
    for copy in copies:
        copy.wait()


def shards(*args):
    (f4, f5, f6, f7, g4, g5, g6, g7, conv_weight, gain, shift, heights, widths) = args
    hbm_spec = pl.BlockSpec(memory_space=pltpu.HBM)
    vmem_spec = pl.BlockSpec(memory_space=pltpu.VMEM)
    feats = (f4, f5, f6, f7)
    vm = pltpu.VMEM
    scratch = (
        [vm((4, 256), F32), vm((4, 256), F32), vm((2, 256), jnp.int32)]
        + [vm(f.shape, BF16) for f in feats]
        + [vm(f.shape, BF16) for f in feats]
        + [
            vm((2304, 256), BF16),
            vm((2304, 256), BF16),
            vm((ROWS, COLS, 256), F32),
            vm((ROWS, COLS, 256), F32),
            vm((ROWS * COLS, 256), F32),
            vm((ROWS * COLS, 768), BF16),
            vm((768, ROWS * COLS), BF16),
            vm((ROWS * COLS, 256), F32),
            vm((ROWS * COLS, 256), F32),
            vm((ROWS * COLS, 256), F32),
            vm(((ROWS + 2) * COLS, 768), BF16),
            vm((ROWS, COLS, 256), F32),
            vm((2, 2, 5, 1, 256), F32),
            vm((2, 5, 1, 256), F32),
            vm((2, 16, 5, 1, 256), F32),
            vm((2, 2, 8, 5, 1, 256), F32),
            vm((9, 256, 256), F32),
            vm((9, 128, 256), F32),
            vm((9, 128, 256), F32),
            vm((3, 9, 32, 256), F32),
            vm((9, 32, 256), F32),
            vm((3, 9, 8, 256), F32),
            vm((8, 9, 1, 256), F32),
            vm((7, 9, 1, 256), F32),
            vm((8, 9, 1, 256), F32),
            pltpu.SemaphoreType.DMA((12,)),
            pltpu.SemaphoreType.DMA((2, 33)),
            pltpu.SemaphoreType.DMA((2, 33)),
            pltpu.SemaphoreType.DMA((len(CHUNKS), 28)),
            pltpu.SemaphoreType.DMA((len(CHUNKS), 28)),
        ]
    )
    results = [f.shape for f in feats] * 2
    shapes = [(shape, BF16) for shape in results] + [((9, 256, 256), F32), ((4, 256), F32), ((4, 256), F32)]
    outs = pl.pallas_call(
        kernel,
        out_shape=[vm(shape, dtype) for shape, dtype in shapes],
        in_specs=[hbm_spec] * 12,
        out_specs=[vmem_spec] * 11,
        scratch_shapes=scratch,
        compiler_params=pltpu.CompilerParams(
            collective_id=0, has_side_effects=True, vmem_limit_bytes=FUSED_VMEM
        ),
        name="fused_step",
    )(
        f4, f5, f6, f7, g4, g5, g6, g7, conv_weight.reshape(2304, 256), gain, shift,
        jnp.broadcast_to(jnp.stack([heights, widths]), (2, 256)),
    )
    outs = pl.pallas_call(
        write_out,
        out_shape=[jax.ShapeDtypeStruct(shape, dtype) for shape, dtype in shapes],
        in_specs=[vmem_spec] * 11,
        out_specs=[hbm_spec] * 11,
        scratch_shapes=[pltpu.SemaphoreType.DMA((11,))],
        compiler_params=pltpu.CompilerParams(vmem_limit_bytes=4 * 1024 * 1024),
        name="write_out",
    )(*outs)
    outs = list(outs)
    outs[8] = outs[8].reshape(3, 3, 256, 256)
    return tuple(outs)


def solution(mesh):
    torus = Mesh(mesh.devices.reshape(NZ, NX, NY, NC), AXES)
    image = P(AXES, None, None, None)
    in_specs = (image,) * 8 + (P(), P(), P(), P(AXES), P(AXES))
    out_specs = (image,) * 8 + (P(), P(), P())
    return jax.shard_map(shards, mesh=torus, in_specs=in_specs, out_specs=out_specs, check_vma=False)
```
